16 devices in a mesh: fsdp: 16 (over z, y, x, core).
Axes of the slice: x: 2, y: 2, z: 2, core: 2. Of those that a mesh axis runs over, the one named last changes fastest.
Arguments:
- token_ids: int32 [512, 512], P('fsdp')
- embed_table: bfloat16 [49152, 960], P('fsdp')
- norm_gain: bfloat16 [960], P('fsdp')
- w_query: bfloat16 [960, 15, 64], P('fsdp')
- w_key: bfloat16 [960, 5, 64], P('fsdp')
- w_value: bfloat16 [960, 5, 64], P('fsdp')
- w_out: bfloat16 [960, 960], P('fsdp')
- grad_out: bfloat16 [512, 512, 960], P('fsdp')
Outputs:
- output 1: bfloat16 [512, 512, 960], P('fsdp')
- output 2: float32 [49152, 960], P('fsdp')
- output 3: float32 [960], P('fsdp')
- output 4: float32 [960, 15, 64], P('fsdp')
- output 5: float32 [960, 5, 64], P('fsdp')
- output 6: float32 [960, 5, 64], P('fsdp')
- output 7: float32 [960, 960], P('fsdp')
All inputs are finite; a program needn't handle non-finite values.
Results may differ from the reference program's by a relative error of at most 0.00861237.
Values are sent between devices in bfloat16 or wider.
A program may use at most 1 GiB of HBM per device.

```python
import jax
import jax.numpy as jnp
from jax import lax

VOCAB_SIZE = 49152
D_MODEL = 960
HEADS = 15
KV_HEADS = 5
HEAD_DIM = 64
GROUP_SIZE = 16
BATCH = 512
SEQ_LEN = 512
CHUNK = 128
ROPE_THETA = 500000.0
NORM_EPS = 1e-5


def setup_inputs(seed: int = 0) -> dict:
    key_list = jax.random.split(jax.random.key(seed), 9)
    first = jax.random.randint(key_list[0], (BATCH, SEQ_LEN), 0, VOCAB_SIZE, dtype=jnp.int32)
    second = jax.random.randint(key_list[1], (BATCH, SEQ_LEN), 0, VOCAB_SIZE, dtype=jnp.int32)
    token_ids = jnp.minimum(first, second).at[0, 0].set(VOCAB_SIZE - 1)
    embed_table = (0.25 * jax.random.normal(key_list[2], (VOCAB_SIZE, D_MODEL), jnp.float32)).astype(jnp.bfloat16)
    norm_gain = (1.0 + 0.3 * jax.random.normal(key_list[3], (D_MODEL,), jnp.float32)).astype(jnp.bfloat16)
    in_scale = D_MODEL ** -0.5
    out_scale = (HEADS * HEAD_DIM) ** -0.5
    w_query = (in_scale * jax.random.normal(key_list[4], (D_MODEL, HEADS, HEAD_DIM), jnp.float32)).astype(jnp.bfloat16)
    w_key = (in_scale * jax.random.normal(key_list[5], (D_MODEL, KV_HEADS, HEAD_DIM), jnp.float32)).astype(jnp.bfloat16)
    w_value = (in_scale * jax.random.normal(key_list[6], (D_MODEL, KV_HEADS, HEAD_DIM), jnp.float32)).astype(jnp.bfloat16)
    w_out = (out_scale * jax.random.normal(key_list[7], (HEADS * HEAD_DIM, D_MODEL), jnp.float32)).astype(jnp.bfloat16)
    grad_out = jax.random.normal(key_list[8], (BATCH, SEQ_LEN, D_MODEL), jnp.float32).astype(jnp.bfloat16)
    return dict(token_ids=token_ids, embed_table=embed_table, norm_gain=norm_gain, w_query=w_query, w_key=w_key, w_value=w_value, w_out=w_out, grad_out=grad_out)


def to_bf16(values):
    return values.astype(jnp.bfloat16).astype(jnp.float32)


def rms_scale(values):
    return values * lax.rsqrt(jnp.mean(values * values, axis=-1, keepdims=True) + NORM_EPS)


def rotary(values):
    half = HEAD_DIM // 2
    frequency = ROPE_THETA ** (-2.0 * jnp.arange(half, dtype=jnp.float32) / HEAD_DIM)
    angles = jnp.arange(SEQ_LEN, dtype=jnp.float32)[:, None] * frequency[None, :]
    cosine = jnp.cos(angles)[:, None, :]
    sine = jnp.sin(angles)[:, None, :]
    first = values[..., :half]
    second = values[..., half:]
    return jnp.concatenate([first * cosine - second * sine, second * cosine + first * sine], axis=-1)


def chunk_attention(query, key_h, value):
    blocks = SEQ_LEN // CHUNK
    group = HEADS // KV_HEADS
    q_blocks = query.reshape(blocks, CHUNK, KV_HEADS, group, HEAD_DIM)
    k_blocks = key_h.reshape(blocks, CHUNK, KV_HEADS, HEAD_DIM)
    v_blocks = value.reshape(blocks, CHUNK, KV_HEADS, HEAD_DIM)
    scores = jnp.einsum('cikgd,cjkd->ckigj', q_blocks, k_blocks) * HEAD_DIM ** -0.5
    causal = jnp.arange(CHUNK)[:, None, None] >= jnp.arange(CHUNK)[None, None, :]
    attn_probs = to_bf16(jax.nn.softmax(jnp.where(causal, scores, -1e30), axis=-1))
    mixed = jnp.einsum('ckigj,cjkd->cikgd', attn_probs, v_blocks)
    return mixed.reshape(SEQ_LEN, HEADS * HEAD_DIM)


def row_forward(x_row, gain, w_query, w_key, w_value, w_out):
    normed = to_bf16(rms_scale(x_row) * gain)
    query = jnp.einsum('sd,dhe->she', normed, w_query)
    key_h = jnp.einsum('sd,dhe->she', normed, w_key)
    value = to_bf16(jnp.einsum('sd,dhe->she', normed, w_value))
    query = to_bf16(rms_scale(rotary(query)))
    key_h = to_bf16(rms_scale(rotary(key_h)))
    mixed = to_bf16(chunk_attention(query, key_h, value))
    return x_row + jnp.dot(mixed, w_out, preferred_element_type=jnp.float32)


def reference(token_ids, embed_table, norm_gain, w_query, w_key, w_value, w_out, grad_out):
    gain32 = norm_gain.astype(jnp.float32)
    query32 = w_query.astype(jnp.float32)
    key32 = w_key.astype(jnp.float32)
    value32 = w_value.astype(jnp.float32)
    wout32 = w_out.astype(jnp.float32)
    param_zero = (jnp.zeros_like(gain32), jnp.zeros_like(query32), jnp.zeros_like(key32), jnp.zeros_like(value32), jnp.zeros_like(wout32))
    table_zero = jnp.zeros((VOCAB_SIZE, D_MODEL), jnp.float32)

    def step(carry, row_inputs):
        table_acc, param_acc = carry
        row_ids, row_cot = row_inputs
        x_row = jnp.take(embed_table, row_ids, axis=0).astype(jnp.float32)
        hidden_row, pullback = jax.vjp(row_forward, x_row, gain32, query32, key32, value32, wout32)
        cotangents = pullback(row_cot.astype(jnp.float32))
        table_acc = table_acc.at[row_ids].add(cotangents[0])
        param_acc = tuple(acc + grad for acc, grad in zip(param_acc, cotangents[1:]))
        return (table_acc, param_acc), hidden_row.astype(jnp.bfloat16)

    (table_acc, param_acc), hidden = lax.scan(step, (table_zero, param_zero), (token_ids, grad_out))
    return (hidden, table_acc / GROUP_SIZE, param_acc[0] / GROUP_SIZE, param_acc[1] / GROUP_SIZE, param_acc[2] / GROUP_SIZE, param_acc[3] / GROUP_SIZE, param_acc[4] / GROUP_SIZE)
```

```python
import functools

import jax
import jax.numpy as jnp
from jax import lax
from jax.experimental import pallas as pl
from jax.experimental.pallas import tpu as pltpu
from jax.sharding import PartitionSpec as P

ROPE_THETA = 500000.0
NORM_EPS = 1e-5
CHUNK_COUNT = 4
LOG2_E = 1.4426950408889634
LANES = 128
F32 = jnp.float32
BF16 = jnp.bfloat16


def dot_nn(a, b):
    return lax.dot_general(a, b, (((1,), (0,)), ((), ())), preferred_element_type=F32)


def dot_nt(a, b):
    return lax.dot_general(a, b, (((1,), (1,)), ((), ())), preferred_element_type=F32)


def rotate_norm(first, second, cosine, sine, inv_dim):
    low = first * cosine - second * sine
    high = second * cosine + first * sine
    mean = jnp.sum(low * low + high * high, axis=0, keepdims=True) * inv_dim
    scale = lax.rsqrt(mean + NORM_EPS)
    return low * scale, high * scale, scale


def rotate_norm_pull(low, high, scale, cosine, sine, d_low, d_high, inv_dim, sm_scale):
    scale = scale * sm_scale
    mean = jnp.sum(low * d_low + high * d_high, axis=0, keepdims=True) * inv_dim
    r_low = (d_low - low * mean) * scale
    r_high = (d_high - high * mean) * scale
    return r_low * cosine + r_high * sine, r_high * cosine - r_low * sine


def block_kernel(sizes, ids_ref, table_ref, dh_ref, wqkv_ref, wqkv_t_ref, wo_ref, wo_t_ref, gain_ref, cos_ref, sin_ref,
                 h_ref, demb_ref, demb_tail_ref, gpack_ref,
                 gqkv_ref, gout_ref, ggain_ref, rows, stage, bias_ref, sems, xt, at, qkv, dmix, mixed, dqkv, dnorm):
    d_model, heads, kv_heads, head_dim, chunk, out_scale, share_rows, padded_rows, pack_columns, _ = sizes
    group = heads // kv_heads
    half = head_dim // 2
    inv_dim = 1.0 / head_dim
    seq_len = rows.shape[1]
    tiles = rows.shape[2]
    chunks = seq_len // chunk
    head_cols = demb_ref.shape[1]
    step = pl.program_id(0)
    last = pl.num_programs(0) - 1
    slot = lax.rem(step, 2)
    next_slot = 1 - slot
    next_base = jnp.minimum(step + 1, last) * seq_len

    def fetch(base, offset, into):
        pltpu.make_async_copy(table_ref.at[ids_ref[base + offset]], rows.at[into, offset], sems.at[into]).start()

    def wait_rows(which):
        pltpu.make_async_copy(table_ref.at[pl.ds(0, seq_len)], rows.at[which], sems.at[which]).wait()
    k_base = heads * head_dim
    v_base = k_base + kv_heads * head_dim
    row_blocks = [(r, min(LANES, d_model - r)) for r in range(0, d_model, LANES)]

    @pl.when(step == 0)
    def _():
        @pl.loop(0, seq_len)
        def _(t):
            fetch(0, t, 0)
        gqkv_ref[...] = jnp.zeros_like(gqkv_ref)
        gout_ref[...] = jnp.zeros_like(gout_ref)
        ggain_ref[...] = jnp.zeros_like(ggain_ref)

    def columns(w):
        return pl.ds(pl.multiple_of(w * chunk, chunk), chunk)

    dmix[...] = dot_nn(wo_ref[...], dh_ref[...]).astype(BF16)
    wait_rows(slot)

    @pl.loop(0, chunks)
    def _(w):
        cols = columns(w)
        stage[...] = rows[slot, cols].astype(F32).reshape(chunk * tiles, LANES)
        total = jnp.zeros((1, chunk), F32)
        for r, n in row_blocks:
            piece = stage[pl.ds(r // LANES, chunk, stride=tiles), :].T[:n]
            xt[r:r + n, cols] = piece
            total += jnp.sum(piece * piece, axis=0, keepdims=True)
        scale = lax.rsqrt(total * (1.0 / d_model) + NORM_EPS)
        for r, n in row_blocks:
            at[r:r + n, cols] = (xt[r:r + n, cols] * scale * gain_ref[r:r + n, :]).astype(BF16)

    qkv[...] = dot_nn(wqkv_t_ref[...], at[...])

    query_pos = lax.broadcasted_iota(jnp.int32, (chunk, chunk), 1)
    key_pos = lax.broadcasted_iota(jnp.int32, (chunk, chunk), 0)
    bias_ref[...] = jnp.where(query_pos >= key_pos, 0.0, -1e30)
    sm_scale = head_dim ** -0.5
    exp2_scale = sm_scale * LOG2_E

    @pl.loop(0, chunks)
    def _(w):
        cols = columns(w)
        cosine = cos_ref[:, cols]
        sine = sin_ref[:, cols]

        def rotated(base):
            return rotate_norm(qkv[base:base + half, cols], qkv[base + half:base + head_dim, cols], cosine, sine, inv_dim)

        everyone = range(kv_heads)
        bias = jnp.concatenate([bias_ref[...]] * group, axis=1)

        def fetch_share(part, parts):
            for t in range(chunk * part // parts, chunk * (part + 1) // parts):
                fetch(next_base, w * chunk + t, next_slot)

        key_parts = [rotated(k_base + kv * head_dim) for kv in everyone]
        key_f = [jnp.concatenate([lo, hi], axis=0) for lo, hi, _ in key_parts]
        key_t = [k.astype(BF16) for k in key_f]
        key = [k.T.astype(BF16) for k in key_f]
        value_f = [qkv[v_base + kv * head_dim:v_base + (kv + 1) * head_dim, cols] for kv in everyone]
        value_t = [v.astype(BF16) for v in value_f]
        value = [v.T.astype(BF16) for v in value_f]
        query_parts = [[rotated((kv * group + g) * head_dim) for g in range(group)] for kv in everyone]
        query_t = [jnp.concatenate([jnp.concatenate([lo, hi], axis=0).astype(BF16) for lo, hi, _ in parts], axis=1)
                   for parts in query_parts]
        dout_t = [jnp.concatenate(
            [dmix[(kv * group + g) * head_dim:(kv * group + g + 1) * head_dim, cols] for g in range(group)], axis=1)
            for kv in everyone]
        scores = [dot_nn(key[kv], query_t[kv]) for kv in everyone]
        d_probs = [dot_nn(value[kv], dout_t[kv]) for kv in everyone]
        weight = [jnp.exp2(scores[kv] * exp2_scale + bias) for kv in everyone]
        probs = [weight[kv] * (1.0 / jnp.sum(weight[kv], axis=0, keepdims=True)) for kv in everyone]
        probs_bf = [p.astype(BF16) for p in probs]
        fetch_share(0, 2)
        out_t = [dot_nn(value_t[kv], probs_bf[kv]).astype(BF16) for kv in everyone]
        d_value = [dot_nt(dout_t[kv], probs_bf[kv]) for kv in everyone]
        delta = [jnp.sum(probs[kv] * d_probs[kv], axis=0, keepdims=True) for kv in everyone]
        dscore_bf = [(probs[kv] * (d_probs[kv] - delta[kv])).astype(BF16) for kv in everyone]
        fetch_share(1, 2)
        d_query = [dot_nn(key_t[kv], dscore_bf[kv]) for kv in everyone]
        d_key = [dot_nt(query_t[kv], dscore_bf[kv]) for kv in everyone]
        for kv in everyone:
            kb = k_base + kv * head_dim
            vb = v_base + kv * head_dim
            for g in range(group):
                base = (kv * group + g) * head_dim
                lanes = slice(g * chunk, (g + 1) * chunk)
                mixed[base:base + head_dim, cols] = out_t[kv][:, lanes]
                lo, hi, scale = query_parts[kv][g]
                d_first, d_second = rotate_norm_pull(
                    lo, hi, scale, cosine, sine, d_query[kv][:half, lanes], d_query[kv][half:, lanes], inv_dim, sm_scale)
                dqkv[base:base + half, cols] = d_first.astype(BF16)
                dqkv[base + half:base + head_dim, cols] = d_second.astype(BF16)
            lo, hi, scale = key_parts[kv]
            d_first, d_second = rotate_norm_pull(
                lo, hi, scale, cosine, sine, d_key[kv][:half], d_key[kv][half:], inv_dim, sm_scale)
            dqkv[kb:kb + half, cols] = d_first.astype(BF16)
            dqkv[kb + half:kb + head_dim, cols] = d_second.astype(BF16)
            dqkv[vb:vb + head_dim, cols] = d_value[kv].astype(BF16)

    h_ref[...] = (xt[...] + dot_nn(wo_t_ref[...], mixed[...])).astype(BF16)
    dnorm[...] = dot_nn(wqkv_ref[...], dqkv[...])
    gout_ref[...] += dot_nt(mixed[...], dh_ref[...])
    gqkv_ref[...] += dot_nt(at[...], dqkv[...])

    @pl.loop(0, chunks, unroll=True)
    def _(w):
        cols = columns(w)
        total = jnp.zeros((1, chunk), F32)
        inner = jnp.zeros((1, chunk), F32)
        for r, n in row_blocks:
            piece = xt[r:r + n, cols]
            total += jnp.sum(piece * piece, axis=0, keepdims=True)
            inner += jnp.sum(piece * (dnorm[r:r + n, cols] * gain_ref[r:r + n, :]), axis=0, keepdims=True)
        scale = lax.rsqrt(total * (1.0 / d_model) + NORM_EPS)
        mean = inner * scale * (1.0 / d_model)
        for r, n in row_blocks:
            unit = xt[r:r + n, cols] * scale
            d_row = dnorm[r:r + n, cols]
            ggain_ref[r:r + n, :] += d_row * unit
            d_x = (d_row * gain_ref[r:r + n, :] - unit * mean) * scale
            full = (dh_ref[r:r + n, cols].astype(F32) + d_x) * out_scale
            if r < head_cols:
                demb_ref[cols, r:r + n] = full.T
            else:
                demb_tail_ref[cols, r - head_cols:r - head_cols + n] = full.T

    @pl.when(step == last)
    def _():
        wait_rows(next_slot)
        gpack_ref[...] = jnp.zeros_like(gpack_ref)

        @pl.loop(0, d_model // (2 * share_rows))
        def _(pair):
            source = pl.ds(pl.multiple_of(pair * 2 * share_rows, 8), 2 * share_rows)
            for grad, column in zip((ggain_ref, gqkv_ref, gout_ref), pack_columns):
                both = grad[source, :]
                for side in range(2):
                    target = pl.ds(pl.multiple_of((2 * pair + side) * padded_rows, 8), share_rows)
                    gpack_ref[target, column:column + grad.shape[1]] = both[side * share_rows:(side + 1) * share_rows]


def fused_block(ids, table, dh_t, wqkv, wqkv_t, wo, wo_t, gain_rows, cos_t, sin_t, sizes, head_cols, interpret=False):
    batch, d_model, seq_len = dh_t.shape
    tokens = batch * seq_len
    tiles = table.shape[1]
    width = wqkv.shape[1]
    mixed_width = wo.shape[0]
    pack_shape = (d_model // sizes[6] * sizes[7], sizes[9])

    def whole(shape):
        return pl.BlockSpec(shape, lambda b, ids: (0,) * len(shape), pipeline_mode=pl.Buffered(buffer_count=1))

    per_token = 2 * (3 * d_model * width + 3 * d_model * mixed_width) + 12 * mixed_width * sizes[4]
    return pl.pallas_call(
        functools.partial(block_kernel, sizes),
        grid_spec=pltpu.PrefetchScalarGridSpec(
            num_scalar_prefetch=1,
            grid=(batch,),
            in_specs=[
                pl.BlockSpec(memory_space=pl.ANY),
                pl.BlockSpec((None, d_model, seq_len), lambda b, ids: (b, 0, 0)),
                whole(wqkv.shape), whole(wqkv_t.shape), whole(wo.shape), whole(wo_t.shape),
                whole(gain_rows.shape), whole(cos_t.shape), whole(sin_t.shape),
            ],
            out_specs=[
                pl.BlockSpec((None, d_model, seq_len), lambda b, ids: (b, 0, 0)),
                pl.BlockSpec((seq_len, head_cols), lambda b, ids: (b, 0)),
                pl.BlockSpec((seq_len, d_model - head_cols), lambda b, ids: (b, 0)),
                whole(pack_shape),
            ],
            scratch_shapes=[
                pltpu.VMEM((d_model, width), F32),
                pltpu.VMEM((mixed_width, d_model), F32),
                pltpu.VMEM((d_model, sizes[4]), F32),
                pltpu.VMEM((2, seq_len, tiles, LANES), BF16),
                pltpu.VMEM((sizes[4] * tiles, LANES), F32),
                pltpu.VMEM((sizes[4], sizes[4]), F32),
                pltpu.SemaphoreType.DMA((2,)),
                pltpu.VMEM((d_model, seq_len), F32),
                pltpu.VMEM((d_model, seq_len), BF16),
                pltpu.VMEM((width, seq_len), F32),
                pltpu.VMEM((mixed_width, seq_len), BF16),
                pltpu.VMEM((mixed_width, seq_len), BF16),
                pltpu.VMEM((width, seq_len), BF16),
                pltpu.VMEM((d_model, seq_len), F32),
            ],
        ),
        out_shape=[
            jax.ShapeDtypeStruct(dh_t.shape, BF16),
            jax.ShapeDtypeStruct((tokens, head_cols), F32),
            jax.ShapeDtypeStruct((tokens, d_model - head_cols), F32),
            jax.ShapeDtypeStruct(pack_shape, F32),
        ],
        compiler_params=pltpu.CompilerParams(dimension_semantics=("arbitrary",), vmem_limit_bytes=60 * 1024 * 1024),
        cost_estimate=pl.CostEstimate(flops=per_token * tokens, bytes_accessed=tokens * d_model * 10, transcendentals=0),
        name="block",
        interpret=interpret,
    )(ids, table, dh_t, wqkv, wqkv_t, wo, wo_t, gain_rows, cos_t, sin_t)


def rotary_tables(seq_len, head_dim):
    half = head_dim // 2
    frequency = ROPE_THETA ** (-2.0 * jnp.arange(half, dtype=F32) / head_dim)
    angles = frequency[:, None] * jnp.arange(seq_len, dtype=F32)[None, :]
    return jnp.cos(angles), jnp.sin(angles)


def solution(mesh):
    group_count = mesh.shape['fsdp']

    def device_step(token_ids, embed_table, norm_gain, w_query, w_key, w_value, w_out, grad_out):
        batch, seq_len = token_ids.shape
        share, d_model = embed_table.shape
        heads, head_dim = w_query.shape[1:]
        kv_heads = w_key.shape[1]
        rows = w_query.shape[0]
        q_width, kv_width = heads * head_dim, kv_heads * head_dim
        width = q_width + 2 * kv_width

        packed = jnp.concatenate([
            w_query.reshape(rows, q_width), w_key.reshape(rows, kv_width), w_value.reshape(rows, kv_width),
            w_out, jnp.broadcast_to(norm_gain[:, None], (rows, LANES))], axis=1)
        weights = lax.all_gather(packed, 'fsdp', axis=0, tiled=True)
        tiles = 8 * pl.cdiv(d_model, 8 * LANES)
        row_tiles = jnp.pad(embed_table, ((0, 0), (0, tiles * LANES - d_model))).reshape(share, tiles, LANES)
        full_table = lax.all_gather(row_tiles, 'fsdp', axis=0, tiled=True)
        wqkv = weights[:, :width]
        wo = weights[:, width:width + d_model]
        gain_rows = weights[:, width + d_model:].astype(F32)
        cos_t, sin_t = rotary_tables(seq_len, head_dim)

        flat_ids = token_ids.reshape(-1)
        head_cols = (d_model // LANES + 1) // 2 * LANES
        chunk = seq_len // CHUNK_COUNT
        qkv_at = LANES
        out_at = qkv_at + pl.cdiv(width, LANES) * LANES
        pack_width = out_at + pl.cdiv(d_model, LANES) * LANES
        padded_rows = pl.cdiv(rows, 8) * 8
        sizes = (d_model, heads, kv_heads, head_dim, chunk, 1.0 / group_count, rows, padded_rows, (0, qkv_at, out_at), pack_width)
        h_t, d_head, d_tail, packed_grads = fused_block(
            flat_ids, full_table, jnp.swapaxes(grad_out, 1, 2), wqkv, wqkv.T, wo, wo.T, gain_rows, cos_t, sin_t, sizes, head_cols)

        grads = lax.psum_scatter(packed_grads, 'fsdp', scatter_dimension=0, tiled=True)[:rows] / group_count
        g_gain = jnp.sum(grads[:, :chunk], axis=1)
        g_qkv = grads[:, qkv_at:qkv_at + width]
        g_out = grads[:, out_at:out_at + d_model]

        def table_share(rows_grad):
            total = jnp.zeros((share * group_count, rows_grad.shape[1]), F32)
            total = total.at[flat_ids].add(rows_grad, mode='promise_in_bounds')
            return lax.psum_scatter(total, 'fsdp', scatter_dimension=0, tiled=True)

        table_grad = jnp.concatenate([table_share(d_head).T, table_share(d_tail).T], axis=0).T
        return (jnp.swapaxes(h_t, 1, 2), table_grad, g_gain,
                g_qkv[:, :q_width].reshape(w_query.shape),
                g_qkv[:, q_width:q_width + kv_width].reshape(w_key.shape),
                g_qkv[:, q_width + kv_width:].reshape(w_value.shape), g_out)

    tokens = P('fsdp', None, None)
    matrix = P('fsdp', None)
    vector = P('fsdp')
    return jax.shard_map(device_step, mesh=mesh, in_specs=(matrix, matrix, vector, tokens, tokens, tokens, matrix, tokens), out_specs=(tokens, matrix, vector, tokens, tokens, tokens, matrix), check_vma=False)
```
